128 devices in a mesh: dp: 16 (over y_hi, x, core), tensor: 8 (over z, y_lo).
Axes of the slice: x: 4, y: 4 (y_hi: 2, y_lo: 2; y = y_hi * 2 + y_lo), z: 4, core: 2. Of those that a mesh axis runs over, the one named last changes fastest.
Arguments:
- tokens: bfloat16 [32768, 1024], P(('dp', 'tensor')), may hold values from -6 to 6
- upstream: bfloat16 [32768, 1024], P(('dp', 'tensor')), may hold values from -6 to 6
- counts: int32 [512], P('dp'), may hold values from 37 to 49, as said below
- norm_gain: float32 [1024], replicated, may hold values from 0.5 to 1.5
- norm_bias: float32 [1024], replicated, may hold values from -4 to 4
- w_qkv: bfloat16 [1024, 3072], P('dp', 'tensor'), may hold values from -0.1875 to 0.1875
- w_out: bfloat16 [1024, 1024], P('tensor', 'dp'), may hold values from -0.1875 to 0.1875
Outputs:
- grad_tokens: bfloat16 [32768, 1024], P(('dp', 'tensor'))
- grad_qkv: float32 [1024, 3072], P('dp', 'tensor')
- grad_out: float32 [1024, 1024], P('tensor', 'dp')
- grad_gain: float32 [1024], replicated
- grad_bias: float32 [1024], replicated
The draws below stay inside these ranges and needn't reach their ends.
Inputs may be any that keep to these rules, and one draw needn't show every extreme that they name: counts[i] is the number of visible tokens of image i, held in its first slots; some image has 49 in every draw.
All inputs are finite; a program needn't handle non-finite values.
Results may differ from the reference program's by a relative error of at most 0.014.
Values may be sent and summed in bfloat16 or wider, within the bound.
A program may use at most 64 MiB of HBM per device.

```python
import jax
import jax.numpy as jnp
from jax import lax

D = 1024
HEADS = 16
HEAD = 64
CAP = 64
MAXC = 49
MINC = 37
IMAGES = 512
TOKENS = 32768


def draw_counts(key, part):
    values = jax.random.randint(key, (IMAGES,), MINC, MAXC + 1, dtype=jnp.int32)
    position = jax.random.randint(jax.random.fold_in(key, 17), (), 0, IMAGES, dtype=jnp.int32)
    return values.at[position].set(MAXC)


def levels(stream_key, dims, cuts, low, high):
    factor_of = 1.0
    for dim, parts in cuts:
        draws = jax.random.uniform(jax.random.fold_in(jax.random.fold_in(stream_key, 6), dim), (parts,), jnp.float32, low / len(cuts), high / len(cuts))
        factor_of = factor_of * jnp.repeat(jnp.exp(draws), dims[dim] // parts).reshape((-1,) + (1,) * (len(dims) - 1 - dim))
    return factor_of


def noise(own_key, extent, scale, reach, cuts=(), kind=jnp.bfloat16):
    loudness = levels(own_key, extent, cuts, -0.22, 0.18) if cuts else 1.0
    values = jax.random.normal(own_key, extent, jnp.float32) * scale * loudness
    return jnp.minimum(jnp.maximum(values, -reach), reach).astype(kind)


def setup_inputs(seed: int = 0) -> dict:
    splits = jax.random.split(jax.random.key(seed), 8)
    return {
        "tokens": noise(splits[0], (TOKENS, D), 1.0, 6.0, ((0, 128),)),
        "upstream": noise(splits[1], (TOKENS, D), 1.0, 6.0, ((0, 128),)),
        "counts": draw_counts(jax.random.fold_in(splits[7], 71), 0),
        "norm_gain": jnp.clip(1.0 + 0.1 * jax.random.normal(splits[3], (D,), jnp.float32), 0.5, 1.5),
        "norm_bias": noise(splits[4], (D,), 1.0, 4.0, (), jnp.float32),
        "w_qkv": noise(splits[5], (D, 3 * D), D ** -0.5, 0.1875, ((0, 16), (1, 8))),
        "w_out": noise(splits[6], (D, D), D ** -0.5, 0.1875, ((0, 8), (1, 16))),
    }


def layer_norm(tokens, norm_gain, norm_bias):
    values = tokens.astype(jnp.float32)
    centre = lax.optimization_barrier(jnp.mean(values, axis=-1, keepdims=True))
    shifted = values - centre
    variance = lax.optimization_barrier(jnp.mean(shifted * shifted, axis=-1, keepdims=True))
    inverse_std = lax.rsqrt(variance + 1e-06)
    scaled = shifted * inverse_std
    normed = (scaled * norm_gain + norm_bias).astype(jnp.bfloat16)
    return (normed, scaled, inverse_std)

def reference(tokens, upstream, counts, norm_gain, norm_bias, w_qkv, w_out):
    total = tokens.shape[0]
    images = total // CAP
    slot_live = jnp.arange(CAP, dtype=jnp.int32)[None, :] < counts[:, None]
    live = slot_live.reshape(-1).astype(jnp.float32)
    normed, scaled, inverse_std = layer_norm(tokens, norm_gain, norm_bias)
    projected = jnp.dot(normed, w_qkv, preferred_element_type=jnp.float32).astype(jnp.bfloat16)
    projected = projected.reshape(images, CAP, HEADS, 3, HEAD)
    query_rows = projected[:, :, :, 0].astype(jnp.float32)
    key_rows = projected[:, :, :, 1].astype(jnp.float32)
    value_rows = projected[:, :, :, 2].astype(jnp.float32)
    score_scale = 1.0 / HEAD ** 0.5
    scores = jnp.einsum('bqhe,bkhe->bhqk', query_rows, key_rows) * score_scale
    scores = jnp.where(slot_live[:, None, None, :], scores, -1e+30)
    probs = jax.nn.softmax(scores, axis=-1)
    probs_low = probs.astype(jnp.bfloat16).astype(jnp.float32)
    attended = jnp.einsum('bhqk,bkhe->bqhe', probs_low, value_rows).astype(jnp.bfloat16).reshape(total, D)
    masked = (upstream.astype(jnp.float32) * live[:, None]).astype(jnp.bfloat16)
    grad_out = lax.dot_general(attended, masked, (((0,), (0,)), ((), ())), preferred_element_type=jnp.float32)
    grad_att = lax.dot_general(masked, w_out, (((1,), (1,)), ((), ())), preferred_element_type=jnp.float32)
    grad_att = grad_att.astype(jnp.bfloat16).reshape(images, CAP, HEADS, HEAD).astype(jnp.float32)
    grad_probs = jnp.einsum('bqhe,bkhe->bhqk', grad_att, value_rows)
    row_delta = lax.optimization_barrier(jnp.sum(probs * grad_probs, axis=-1, keepdims=True))
    grad_scores = (probs * (grad_probs - row_delta) * score_scale).astype(jnp.bfloat16).astype(jnp.float32)
    grad_value = jnp.einsum('bhqk,bqhe->bkhe', probs_low, grad_att).astype(jnp.bfloat16)
    grad_query = jnp.einsum('bhqk,bkhe->bqhe', grad_scores, key_rows).astype(jnp.bfloat16)
    grad_key = jnp.einsum('bhqk,bqhe->bkhe', grad_scores, query_rows).astype(jnp.bfloat16)
    grad_proj = jnp.stack([grad_query, grad_key, grad_value], axis=3).reshape(total, 3 * D)
    grad_qkv = lax.dot_general(normed, grad_proj, (((0,), (0,)), ((), ())), preferred_element_type=jnp.float32)
    grad_normed = lax.dot_general(grad_proj, w_qkv, (((1,), (1,)), ((), ())), preferred_element_type=jnp.float32)
    grad_gain = lax.optimization_barrier(jnp.sum(grad_normed * scaled, axis=0))
    grad_bias = lax.optimization_barrier(jnp.sum(grad_normed, axis=0))
    grad_scaled = grad_normed * norm_gain
    grad_ln = inverse_std * (grad_scaled - lax.optimization_barrier(jnp.mean(grad_scaled, axis=-1, keepdims=True)) - scaled * lax.optimization_barrier(jnp.mean(grad_scaled * scaled, axis=-1, keepdims=True)))
    grad_tokens = (upstream.astype(jnp.float32) * live[:, None] + grad_ln).astype(jnp.bfloat16)
    return (grad_tokens, grad_qkv, grad_out, grad_gain, grad_bias)
```

```python
import functools

import jax
import jax.numpy as jnp
from jax import lax
from jax.experimental import pallas as pl
from jax.experimental.pallas import tpu as pltpu
from jax.sharding import Mesh
from jax.sharding import PartitionSpec as P

D = 1024
HEAD = 64
CAP = 64
TENSOR = ("tensor_0", "tensor_1")
DP = ("dp_0", "dp_1", "dp_2")
DP_TENSOR = ("dp_0", "dp_1", "dp_2", "tensor_0", "tensor_1")
MESH = pl.DeviceIdType.MESH
F32 = jnp.float32
BF16 = jnp.bfloat16

ROWS = (48, 48, 48, 48, 32, 32)
FIRST = (0, 48, 96, 144, 192, 224)
COLOURS = 6
BITS = 6
BASE = ("x0", "y0", "z0", "x1", "y1", "z1")


def order(colour):
    return [BASE[(colour + s) % BITS] for s in range(BITS)]


def gray(x, y, z):
    return {
        "x0": ((x + 1) // 2) % 2,
        "x1": x // 2,
        "y0": ((y + 1) // 2) % 2,
        "y1": y // 2,
        "z0": ((z + 1) // 2) % 2,
        "z1": z // 2,
    }


def bits_of(place, colour):
    return [place[name] for name in order(colour)]


def joined(bits):
    total = 0
    for s, bit in enumerate(bits):
        total = total + bit * (1 << s)
    return total


def held(bits, p):
    if p == 0:
        return joined(bits), 1
    own = [0] * (p - 1) + [1 - bits[p - 1]] + list(bits[p:])
    return joined(own), 1 << (p - 1)


def across(bits, s):
    return list(bits[:s]) + [1 - bits[s]] + list(bits[s + 1 :])


PIECE_AT = []
_at = 0
for _p in range(BITS):
    PIECE_AT.append(_at)
    _at += (BITS - _p) * max(1, (1 << _p) // 2)
BLOCKS = 1 << BITS


def dot(a, b, dims):
    return lax.dot_general(a, b, (dims, ((), ())), preferred_element_type=F32)


def kernel(
    tok_ref,
    up_ref,
    counts_ref,
    gain_ref,
    bias_ref,
    wq_ref,
    wo_ref,
    dtok_ref,
    dq_ref,
    do_ref,
    dgain_ref,
    dbias_ref,
    *scratch,
):
    w_bufs = scratch[0:6]
    g_bufs = scratch[6:12]
    q_bufs = scratch[12:18]
    (
        mine,
        theirs,
        x_ref,
        u_ref,
        live_ref,
        xhat_ref,
        rstd_ref,
        wt_ref,
        wot_ref,
        proj_ref,
        gatt_ref,
        att_ref,
        gproj_ref,
        gn_own,
        gn_out,
        gn_in,
        sum_ref,
        sum_in,
        last_own,
        last_in,
        ag_send,
        ag_recv,
        rs_send,
        rs_recv,
        pair_send,
        pair_recv,
        sum_send,
        sum_recv,
    ) = scratch[18:]

    yh, x, c = (lax.axis_index(name) for name in DP)
    z, yl = (lax.axis_index(name) for name in TENSOR)
    y = 2 * yh + yl
    place = gray(x, y, z)
    peer = {
        "x0": {"dp_1": x + 1 - 2 * (x % 2)},
        "x1": {"dp_1": 3 - x},
        "y0": {"tensor_1": 1 - yl},
        "y1": {"dp_0": 1 - yh, "tensor_1": 1 - yl},
        "z0": {"tensor_0": z + 1 - 2 * (z % 2)},
        "z1": {"tensor_0": 3 - z},
        "c": {"dp_2": 1 - c},
    }
    bits = [bits_of(place, k) for k in range(COLOURS)]

    barrier = pltpu.get_barrier_semaphore()
    for name in peer:
        pl.semaphore_signal(barrier, inc=1, device_id=peer[name], device_id_type=MESH)

    def remote(src, dst, send, recv, name):
        return pltpu.make_async_remote_copy(
            src_ref=src,
            dst_ref=dst,
            send_sem=send,
            recv_sem=recv,
            device_id=peer[name],
            device_id_type=MESH,
        )

    def pair_copy(i, src, dst):
        return remote(src, dst, pair_send.at[i], pair_recv.at[i], "c")

    wq_t = wq_ref[...].astype(F32).T
    wo_f = wo_ref[...].astype(F32)
    for h in range(2):
        part = jnp.concatenate(
            [wq_t[192 * h : 192 * (h + 1)], wo_f[64 * h : 64 * (h + 1)]], axis=0
        )
        mine[h] = jnp.concatenate([part, part], axis=1).astype(BF16)

    pl.semaphore_wait(barrier, len(peer))
    first = pair_copy(0, mine.at[1 - c], theirs)
    first.start()
    first.wait()
    lane = lax.broadcasted_iota(jnp.int32, (256, 128), 1)
    own_half = (lane < 64) == (c == 0)
    block = jnp.where(own_half, mine[c].astype(F32), theirs[...].astype(F32)).astype(BF16)
    for k in range(COLOURS):
        w_bufs[k][joined(bits[k])] = block[FIRST[k] : FIRST[k] + ROWS[k]]

    def ag_copy(k, s, p):
        at, n = held(bits[k], p)
        part = w_bufs[k].at[pl.ds(at, n)]
        return remote(part, part, ag_send.at[k], ag_recv.at[k, s], order(k)[s])

    def ag_sends(p):
        for k in range(COLOURS):
            if p > 0:
                at, n = held(bits[k], p)
                part = w_bufs[k].at[pl.ds(at, n)]
                pltpu.make_async_copy(part, part, ag_recv.at[k, p - 1]).wait()
            if p < BITS:
                ag_copy(k, p, p).start()
        for s in range(p + 1, BITS):
            for k in range(COLOURS):
                ag_copy(k, s, p).start()

    ag_sends(0)

    values = tok_ref[...].astype(F32)
    centre = jnp.mean(values, axis=-1, keepdims=True)
    shifted = values - centre
    variance = jnp.mean(shifted * shifted, axis=-1, keepdims=True)
    inverse = lax.rsqrt(variance + 1e-6)
    scaled = shifted * inverse
    xhat_ref[...] = scaled
    rstd_ref[...] = jnp.broadcast_to(inverse, (256, 128))
    own_rows = pl.ds(pl.multiple_of(c * 256, 256), 256)
    x_ref[own_rows, :] = (scaled * gain_ref[...] + bias_ref[...]).astype(BF16)
    start = (2 * z + yl) * 4
    row = lax.broadcasted_iota(jnp.int32, (256, 128), 0)
    image = row // CAP
    count = jnp.where(
        image < 2,
        jnp.where(image == 0, counts_ref[start], counts_ref[start + 1]),
        jnp.where(image == 2, counts_ref[start + 2], counts_ref[start + 3]),
    )
    live = jnp.where(row % CAP < count, 1.0, 0.0).astype(F32)
    live_ref[own_rows, :] = live
    u_ref[own_rows, :] = (up_ref[...].astype(F32) * live[:, :1]).astype(BF16)
    shared = [
        pair_copy(1, x_ref.at[own_rows], x_ref.at[own_rows]),
        pair_copy(2, u_ref.at[own_rows], u_ref.at[own_rows]),
        pair_copy(3, live_ref.at[own_rows], live_ref.at[own_rows]),
    ]
    for copy in shared:
        copy.start()

    for p in range(1, BITS + 1):
        ag_sends(p)

    def block_at(k, zz, yy, xx):
        return joined(bits_of(gray(xx, yy, zz), k))

    @pl.loop(0, 4)
    def _(zz):
        for yy in range(4):
            t_rows = pl.multiple_of((2 * zz + yy % 2) * 192, 192)
            o_rows = pl.multiple_of((2 * zz + yy % 2) * 64, 64)
            for xx in range(4):
                at = ((yy // 2) * 4 + xx) * 128
                for k in range(4):
                    wt_ref[pl.ds(t_rows + FIRST[k], 48), at : at + 128] = w_bufs[k][
                        block_at(k, zz, yy, xx)
                    ]
                for k in range(4, 6):
                    wot_ref[pl.ds(o_rows + FIRST[k] - 192, 32), at : at + 128] = w_bufs[k][
                        block_at(k, zz, yy, xx)
                    ]

    for copy in shared:
        copy.wait()

    @pl.loop(0, 4)
    def _(i):
        rows = pl.ds(pl.multiple_of(i * 384, 384), 384)
        proj_ref[rows, :] = dot(wt_ref[rows, :], x_ref[...], ((1,), (1,))).astype(BF16)

    @pl.loop(0, 2)
    def _(i):
        rows = pl.ds(pl.multiple_of(i * 256, 256), 256)
        gatt_ref[rows, :] = dot(wot_ref[rows, :], u_ref[...], ((1,), (1,))).astype(BF16)

    left = lax.broadcasted_iota(jnp.int32, (64, 128), 1) < 64

    def folded(a):
        return jnp.where(left, a[:64], a[64:])

    def unfolded(a):
        zero = jnp.zeros_like(a)
        return jnp.concatenate([jnp.where(left, a, zero), jnp.where(left, zero, a)], axis=0).astype(
            BF16
        )

    @pl.loop(0, 8)
    def _(t):
        base = pl.multiple_of(t * 192, 192)
        o_base = pl.multiple_of(t * 64, 64)
        for pair in range(4):
            lanes = slice(pair * 128, pair * 128 + 128)
            q = proj_ref[pl.ds(base, 64), lanes]
            k = proj_ref[pl.ds(base + 64, 64), lanes]
            v = proj_ref[pl.ds(base + 128, 64), lanes]
            g = gatt_ref[pl.ds(o_base, 64), lanes]
            key_live = folded(live_ref[lanes, :]) > 0.5
            scores = folded(dot(k, q, ((0,), (0,)))) * 0.125
            scores = jnp.where(key_live, scores, -1e30)
            top = jnp.max(scores, axis=0, keepdims=True)
            powers = jnp.exp(scores - top)
            probs = powers / jnp.sum(powers, axis=0, keepdims=True)
            grad_probs = folded(dot(v, g, ((0,), (0,))))
            delta = jnp.sum(probs * grad_probs, axis=0, keepdims=True)
            grad_scores = unfolded(probs * (grad_probs - delta) * 0.125)
            probs_low = unfolded(probs)
            att_ref[pl.ds(o_base, 64), lanes] = dot(v, probs_low, ((1,), (0,))).astype(BF16)
            gproj_ref[pl.ds(base, 64), lanes] = dot(k, grad_scores, ((1,), (0,))).astype(BF16)
            gproj_ref[pl.ds(base + 64, 64), lanes] = dot(q, grad_scores, ((1,), (1,))).astype(BF16)
            gproj_ref[pl.ds(base + 128, 64), lanes] = dot(g, probs_low, ((1,), (1,))).astype(BF16)

    @pl.loop(0, 4)
    def _(zz):
        o_rows = pl.ds(pl.multiple_of(zz * 128, 128), 128)
        t_rows = pl.ds(pl.multiple_of(zz * 384, 384), 384)
        out = dot(att_ref[o_rows, :], u_ref[...], ((1,), (0,))).astype(BF16)
        for yy in range(4):
            for xx in range(4):
                at = ((yy // 2) * 4 + xx) * 128
                for k in range(4, 6):
                    low = (yy % 2) * 64 + FIRST[k] - 192
                    g_bufs[k][block_at(k, zz, yy, xx)] = out[low : low + 32, at : at + 128]
        out = dot(gproj_ref[t_rows, :], x_ref[...], ((1,), (0,))).astype(BF16)
        for yy in range(4):
            for xx in range(4):
                at = ((yy // 2) * 4 + xx) * 128
                for k in range(4):
                    low = (yy % 2) * 192 + FIRST[k]
                    g_bufs[k][block_at(k, zz, yy, xx)] = out[low : low + 48, at : at + 128]

    def q_part(k, p, s, count):
        n = max(1, (1 << p) // 2)
        return q_bufs[k].at[pl.ds(PIECE_AT[p] + (s - p) * n, count * n)]

    def rs_sends(s):
        for p in range(s, -1, -1):
            for k in range(COLOURS):
                at, n = held(across(bits[k], s), p)
                remote(
                    g_bufs[k].at[pl.ds(at, n)],
                    q_part(k, p, s, 1),
                    rs_send.at[k],
                    rs_recv.at[k, p],
                    order(k)[s],
                ).start()

    rs_sends(BITS - 1)

    for other in range(2):
        for half in range(2):
            rows = pl.ds(
                pl.multiple_of((c if other == 0 else 1 - c) * 256 + half * 128, 128), 128
            )
            part = dot(gproj_ref[:, rows], wt_ref[...], ((0,), (0,)))
            if other == 0:
                gn_own[half * 128 : half * 128 + 128] = part
            else:
                gn_out[half * 128 : half * 128 + 128] = part.astype(BF16)
    swap = pair_copy(4, gn_out, gn_in)
    swap.start()

    def sum_step(i, name):
        return remote(sum_ref.at[i], sum_in.at[i], sum_send.at[i], sum_recv.at[i], name)

    def sum_finish(i, name):
        sum_step(i, name).wait_recv()
        sum_ref[i + 1] = sum_ref[i] + sum_in[i]

    names = ("c",) + BASE
    for s in range(BITS - 2, -1, -1):
        p = s + 1
        for k in range(COLOURS):
            at, n = held(bits[k], p)
            count = BITS - p
            whole = q_part(k, p, p, count)
            pltpu.make_async_copy(whole, whole, rs_recv.at[k, p]).wait()

            def add(i, _, k=k, p=p, n=n, at=at, count=count):
                total = g_bufs[k][at + i].astype(F32)
                for j in range(count):
                    total = total + q_bufs[k][PIECE_AT[p] + j * n + i].astype(F32)
                g_bufs[k][at + i] = total.astype(BF16)
                return 0

            lax.fori_loop(0, n, add, 0)
        rs_sends(s)
        if s == BITS - 2:
            swap.wait()
            live_own = live_ref[own_rows, :][:, :1]
            scaled = xhat_ref[...]
            grad_normed = gn_own[...] + gn_in[...].astype(F32)
            sum_ref[0] = jnp.concatenate(
                [
                    jnp.sum(grad_normed * scaled, axis=0, keepdims=True),
                    jnp.sum(grad_normed, axis=0, keepdims=True),
                ],
                axis=0,
            )
            sum_step(0, names[0]).start()
            g = grad_normed * gain_ref[...]
            grad_ln = rstd_ref[...][:, :1] * (
                g
                - jnp.mean(g, axis=-1, keepdims=True)
                - scaled * jnp.mean(g * scaled, axis=-1, keepdims=True)
            )
            dtok_ref[...] = (up_ref[...].astype(F32) * live_own + grad_ln).astype(BF16)
        else:
            i = BITS - 3 - s
            sum_finish(i, names[i])
            sum_step(i + 1, names[i + 1]).start()
    for k in range(COLOURS):
        whole = q_part(k, 0, 0, BITS)
        pltpu.make_async_copy(whole, whole, rs_recv.at[k, 0]).wait()
        total = g_bufs[k][joined(bits[k])].astype(F32)
        for s in range(BITS):
            total = total + q_bufs[k][s].astype(F32)
        last_own[FIRST[k] : FIRST[k] + ROWS[k]] = total
    final = pair_copy(5, last_own, last_in)
    final.start()
    for i in range(BITS - 2, 7):
        sum_finish(i, names[i])
        if i < 6:
            sum_step(i + 1, names[i + 1]).start()
        if i == BITS - 2:
            final.wait()
            for h in range(2):
                blk = jnp.where(c == h, last_own[...], last_in[...])
                blk = jnp.where(c == 0, blk, pltpu.roll(blk, 64, 1))[:, :64]
                dq_ref[:, 192 * h : 192 * (h + 1)] = blk[:192].T
                do_ref[64 * h : 64 * (h + 1), :] = blk[192:]
    dgain_ref[...] = sum_ref[7, 0:1]
    dbias_ref[...] = sum_ref[7, 1:2]
    for i in range(7):
        sum_step(i, names[i]).wait_send()
    for k in range(COLOURS):
        for bufs, sems in ((w_bufs, ag_send), (g_bufs, rs_send)):
            part = bufs[k].at[pl.ds(0, BLOCKS - 1)]
            pltpu.make_async_copy(part, part, sems.at[k]).wait()


def on_device(tokens, upstream, counts, norm_gain, norm_bias, w_qkv, w_out):
    vmem = pl.BlockSpec(memory_space=pltpu.VMEM)
    blocks = [pltpu.VMEM((BLOCKS, r, 128), BF16) for r in ROWS]
    parts = [pltpu.VMEM((BLOCKS - 1, r, 128), BF16) for r in ROWS]
    dma = pltpu.SemaphoreType.DMA
    outs = pl.pallas_call(
        kernel,
        out_shape=(
            jax.ShapeDtypeStruct((256, D), BF16),
            jax.ShapeDtypeStruct((64, 384), F32),
            jax.ShapeDtypeStruct((128, 64), F32),
            jax.ShapeDtypeStruct((1, D), F32),
            jax.ShapeDtypeStruct((1, D), F32),
        ),
        in_specs=[vmem, vmem, pl.BlockSpec(memory_space=pltpu.SMEM)] + [vmem] * 4,
        out_specs=(vmem,) * 5,
        scratch_shapes=[
            *blocks,
            *blocks,
            *parts,
            pltpu.VMEM((2, 256, 128), BF16),
            pltpu.VMEM((256, 128), BF16),
            pltpu.VMEM((512, D), BF16),
            pltpu.VMEM((512, D), BF16),
            pltpu.VMEM((512, 128), F32),
            pltpu.VMEM((256, D), F32),
            pltpu.VMEM((256, 128), F32),
            pltpu.VMEM((1536, D), BF16),
            pltpu.VMEM((512, D), BF16),
            pltpu.VMEM((1536, 512), BF16),
            pltpu.VMEM((512, 512), BF16),
            pltpu.VMEM((512, 512), BF16),
            pltpu.VMEM((1536, 512), BF16),
            pltpu.VMEM((256, D), F32),
            pltpu.VMEM((256, D), BF16),
            pltpu.VMEM((256, D), BF16),
            pltpu.VMEM((8, 2, D), F32),
            pltpu.VMEM((7, 2, D), F32),
            pltpu.VMEM((256, 128), F32),
            pltpu.VMEM((256, 128), F32),
            dma((COLOURS,)),
            dma((COLOURS, BITS)),
            dma((COLOURS,)),
            dma((COLOURS, BITS)),
            dma((6,)),
            dma((6,)),
            dma((7,)),
            dma((7,)),
        ],
        compiler_params=pltpu.CompilerParams(
            collective_id=0, has_side_effects=True, vmem_limit_bytes=60 * 1024 * 1024
        ),
    )(
        tokens,
        upstream,
        counts,
        norm_gain.reshape(1, D),
        norm_bias.reshape(1, D),
        w_qkv,
        w_out,
    )
    dtok, dq, do, dgain, dbias = outs
    return dtok, dq, do, dgain.reshape(D), dbias.reshape(D)


def solution(mesh):
    finer = Mesh(
        mesh.devices.reshape(2, 4, 2, 4, 2), ("dp_0", "dp_1", "dp_2", "tensor_0", "tensor_1")
    )
    in_specs = (
        P(DP_TENSOR, None),
        P(DP_TENSOR, None),
        P(DP),
        P(),
        P(),
        P(DP, TENSOR),
        P(TENSOR, DP),
    )
    out_specs = (P(DP_TENSOR, None), P(DP, TENSOR), P(TENSOR, DP), P(), P())
    return jax.shard_map(
        on_device, mesh=finer, in_specs=in_specs, out_specs=out_specs, check_vma=False
    )
```

```python
import functools

import jax
import jax.numpy as jnp
from jax import lax
from jax.experimental import pallas as pl
from jax.experimental.pallas import tpu as pltpu
from jax.sharding import Mesh
from jax.sharding import PartitionSpec as P

D = 1024
HEAD = 64
CAP = 64
TENSOR = ("tensor_0", "tensor_1")
DP = ("dp_0", "dp_1", "dp_2")
DP_TENSOR = ("dp_0", "dp_1", "dp_2", "tensor_0", "tensor_1")
MESH = pl.DeviceIdType.MESH
F32 = jnp.float32
BF16 = jnp.bfloat16

ROWS = (48, 48, 48, 48, 32, 32)
FIRST = (0, 48, 96, 144, 192, 224)
COLOURS = 6
BITS = 6
BASE = ("x0", "y0", "z0", "x1", "y1", "z1")


def order(colour):
    return [BASE[(colour + s) % BITS] for s in range(BITS)]


def gray(x, y, z):
    return {
        "x0": ((x + 1) // 2) % 2,
        "x1": x // 2,
        "y0": ((y + 1) // 2) % 2,
        "y1": y // 2,
        "z0": ((z + 1) // 2) % 2,
        "z1": z // 2,
    }


def bits_of(place, colour):
    return [place[name] for name in order(colour)]


def joined(bits):
    total = 0
    for s, bit in enumerate(bits):
        total = total + bit * (1 << s)
    return total


def held(bits, p):
    if p == 0:
        return joined(bits), 1
    own = [0] * (p - 1) + [1 - bits[p - 1]] + list(bits[p:])
    return joined(own), 1 << (p - 1)


def across(bits, s):
    return list(bits[:s]) + [1 - bits[s]] + list(bits[s + 1 :])


PIECE_AT = []
_at = 0
for _p in range(BITS):
    PIECE_AT.append(_at)
    _at += (BITS - _p) * max(1, (1 << _p) // 2)
BLOCKS = 1 << BITS


def dot(a, b, dims):
    return lax.dot_general(a, b, (dims, ((), ())), preferred_element_type=F32)


def kernel(
    tok_in,
    up_in,
    counts_in,
    gain_in,
    bias_in,
    wq_in,
    wo_in,
    dtok_out,
    last_ref,
    sums_ref,
    *scratch,
):
    w_bufs = scratch[0:6]
    g_bufs = scratch[6:12]
    q_bufs = scratch[12:18]
    (
        mine,
        theirs,
        x_ref,
        u_ref,
        live_ref,
        xhat_ref,
        rstd_ref,
        wt_ref,
        wot_ref,
        proj_ref,
        gatt_ref,
        att_ref,
        gproj_ref,
        gn_own,
        gn_out,
        gn_in,
        sum_ref,
        sum_in,
        last_own,
        last_in,
        ag_send,
        ag_recv,
        rs_send_sem,
        rs_recv,
        pair_send,
        pair_recv,
        sum_send,
        sum_recv,
        tok_ref,
        up_ref,
        wq_ref,
        wo_ref,
        gain_ref,
        bias_ref,
        counts_ref,
        dtok_ref,
        load_sem,
    ) = scratch[18:]

    loads = [
        pltpu.make_async_copy(wq_in, wq_ref, load_sem.at[0]),
        pltpu.make_async_copy(wo_in, wo_ref, load_sem.at[1]),
        pltpu.make_async_copy(tok_in, tok_ref, load_sem.at[2]),
        pltpu.make_async_copy(up_in, up_ref, load_sem.at[3]),
        pltpu.make_async_copy(gain_in, gain_ref, load_sem.at[4]),
        pltpu.make_async_copy(bias_in, bias_ref, load_sem.at[5]),
        pltpu.make_async_copy(counts_in, counts_ref, load_sem.at[6]),
    ]
    for load in loads:
        load.start()

    yh, x, c = (lax.axis_index(name) for name in DP)
    z, yl = (lax.axis_index(name) for name in TENSOR)
    y = 2 * yh + yl
    place = gray(x, y, z)
    peer = {
        "x0": {"dp_1": x + 1 - 2 * (x % 2)},
        "x1": {"dp_1": 3 - x},
        "y0": {"tensor_1": 1 - yl},
        "y1": {"dp_0": 1 - yh, "tensor_1": 1 - yl},
        "z0": {"tensor_0": z + 1 - 2 * (z % 2)},
        "z1": {"tensor_0": 3 - z},
        "c": {"dp_2": 1 - c},
    }
    bits = [bits_of(place, k) for k in range(COLOURS)]

    barrier = pltpu.get_barrier_semaphore()
    for name in peer:
        pl.semaphore_signal(barrier, inc=1, device_id=peer[name], device_id_type=MESH)

    def remote(src, dst, send, recv, name):
        return pltpu.make_async_remote_copy(
            src_ref=src,
            dst_ref=dst,
            send_sem=send,
            recv_sem=recv,
            device_id=peer[name],
            device_id_type=MESH,
        )

    def pair_copy(i, src, dst):
        return remote(src, dst, pair_send.at[i], pair_recv.at[i], "c")

    loads[0].wait()
    loads[1].wait()
    wq_t = wq_ref[...].astype(F32).T
    wo_f = wo_ref[...].astype(F32).T
    for h in range(2):
        part = jnp.concatenate(
            [wq_t[192 * h : 192 * (h + 1)], wo_f[64 * h : 64 * (h + 1)]], axis=0
        )
        mine[h] = jnp.concatenate([part, part], axis=1).astype(BF16)

    pl.semaphore_wait(barrier, len(peer))
    first = pair_copy(0, mine.at[1 - c], theirs)
    first.start()
    first.wait()
    lane = lax.broadcasted_iota(jnp.int32, (256, 128), 1)
    own_half = (lane < 64) == (c == 0)
    block = jnp.where(own_half, mine[c].astype(F32), theirs[...].astype(F32)).astype(BF16)
    for k in range(COLOURS):
        w_bufs[k][joined(bits[k])] = block[FIRST[k] : FIRST[k] + ROWS[k]]

    def ag_copy(k, s, p):
        at, n = held(bits[k], p)
        part = w_bufs[k].at[pl.ds(at, n)]
        return remote(part, part, ag_send.at[k], ag_recv.at[k, s], order(k)[s])

    def ag_sends(p):
        for k in range(COLOURS):
            if p > 0:
                at, n = held(bits[k], p)
                part = w_bufs[k].at[pl.ds(at, n)]
                pltpu.make_async_copy(part, part, ag_recv.at[k, p - 1]).wait()
            if p < BITS:
                ag_copy(k, p, p).start()
        for s in range(p + 1, BITS):
            for k in range(COLOURS):
                ag_copy(k, s, p).start()

    ag_sends(0)

    for load in loads[2:]:
        load.wait()
    values = tok_ref[...].astype(F32)
    centre = jnp.mean(values, axis=-1, keepdims=True)
    shifted = values - centre
    variance = jnp.mean(shifted * shifted, axis=-1, keepdims=True)
    inverse = lax.rsqrt(variance + 1e-6)
    scaled = shifted * inverse
    xhat_ref[...] = scaled
    rstd_ref[...] = jnp.broadcast_to(inverse, (256, 128))
    own_rows = pl.ds(pl.multiple_of(c * 256, 256), 256)
    x_ref[own_rows, :] = (scaled * gain_ref[...] + bias_ref[...]).astype(BF16)
    start = (2 * z + yl) * 4
    row = lax.broadcasted_iota(jnp.int32, (256, 128), 0)
    image = row // CAP
    count = jnp.where(
        image < 2,
        jnp.where(image == 0, counts_ref[start], counts_ref[start + 1]),
        jnp.where(image == 2, counts_ref[start + 2], counts_ref[start + 3]),
    )
    live = jnp.where(row % CAP < count, 1.0, 0.0).astype(F32)
    live_ref[own_rows, :] = live
    u_ref[own_rows, :] = (up_ref[...].astype(F32) * live[:, :1]).astype(BF16)
    shared = [
        pair_copy(1, x_ref.at[own_rows], x_ref.at[own_rows]),
        pair_copy(2, u_ref.at[own_rows], u_ref.at[own_rows]),
        pair_copy(3, live_ref.at[own_rows], live_ref.at[own_rows]),
    ]
    for copy in shared:
        copy.start()

    for p in range(1, BITS + 1):
        ag_sends(p)

    def block_at(k, zz, yy, xx):
        return joined(bits_of(gray(xx, yy, zz), k))

    @pl.loop(0, 4)
    def _(zz):
        for yy in range(4):
            t_rows = pl.multiple_of((2 * zz + yy % 2) * 192, 192)
            o_rows = pl.multiple_of((2 * zz + yy % 2) * 64, 64)
            for xx in range(4):
                at = ((yy // 2) * 4 + xx) * 128
                for k in range(4):
                    wt_ref[pl.ds(t_rows + FIRST[k], 48), at : at + 128] = w_bufs[k][
                        block_at(k, zz, yy, xx)
                    ]
                for k in range(4, 6):
                    wot_ref[pl.ds(o_rows + FIRST[k] - 192, 32), at : at + 128] = w_bufs[k][
                        block_at(k, zz, yy, xx)
                    ]

    for copy in shared:
        copy.wait()

    @pl.loop(0, 4)
    def _(i):
        rows = pl.ds(pl.multiple_of(i * 384, 384), 384)
        proj_ref[rows, :] = dot(wt_ref[rows, :], x_ref[...], ((1,), (1,))).astype(BF16)

    @pl.loop(0, 2)
    def _(i):
        rows = pl.ds(pl.multiple_of(i * 256, 256), 256)
        gatt_ref[rows, :] = dot(wot_ref[rows, :], u_ref[...], ((1,), (1,))).astype(BF16)

    left = lax.broadcasted_iota(jnp.int32, (64, 128), 1) < 64

    def folded(a):
        return jnp.where(left, a[:64], a[64:])

    def unfolded(a):
        zero = jnp.zeros_like(a)
        return jnp.concatenate([jnp.where(left, a, zero), jnp.where(left, zero, a)], axis=0).astype(
            BF16
        )

    @pl.loop(0, 8)
    def _(t):
        base = pl.multiple_of(t * 192, 192)
        o_base = pl.multiple_of(t * 64, 64)
        for pair in range(4):
            lanes = slice(pair * 128, pair * 128 + 128)
            q = proj_ref[pl.ds(base, 64), lanes]
            k = proj_ref[pl.ds(base + 64, 64), lanes]
            v = proj_ref[pl.ds(base + 128, 64), lanes]
            g = gatt_ref[pl.ds(o_base, 64), lanes]
            key_live = folded(live_ref[lanes, :]) > 0.5
            scores = folded(dot(k, q, ((0,), (0,)))) * 0.125
            scores = jnp.where(key_live, scores, -1e30)
            top = jnp.max(scores, axis=0, keepdims=True)
            powers = jnp.exp(scores - top)
            probs = powers / jnp.sum(powers, axis=0, keepdims=True)
            grad_probs = folded(dot(v, g, ((0,), (0,))))
            delta = jnp.sum(probs * grad_probs, axis=0, keepdims=True)
            grad_scores = unfolded(probs * (grad_probs - delta) * 0.125)
            probs_low = unfolded(probs)
            att_ref[pl.ds(o_base, 64), lanes] = dot(v, probs_low, ((1,), (0,))).astype(BF16)
            gproj_ref[pl.ds(base, 64), lanes] = dot(k, grad_scores, ((1,), (0,))).astype(BF16)
            gproj_ref[pl.ds(base + 64, 64), lanes] = dot(q, grad_scores, ((1,), (1,))).astype(BF16)
            gproj_ref[pl.ds(base + 128, 64), lanes] = dot(g, probs_low, ((1,), (1,))).astype(BF16)

    swap = pair_copy(4, gn_out, gn_in)
    for other in (1, 0):
        for half in range(2):
            rows = pl.ds(
                pl.multiple_of((c if other == 0 else 1 - c) * 256 + half * 128, 128), 128
            )
            part = dot(gproj_ref[:, rows], wt_ref[...], ((0,), (0,)))
            if other == 0:
                gn_own[half * 128 : half * 128 + 128] = part
            else:
                gn_out[half * 128 : half * 128 + 128] = part.astype(BF16)
        if other == 1:
            swap.start()

    @pl.loop(0, 4)
    def _(zz):
        o_rows = pl.ds(pl.multiple_of(zz * 128, 128), 128)
        t_rows = pl.ds(pl.multiple_of(zz * 384, 384), 384)
        out = dot(att_ref[o_rows, :], u_ref[...], ((1,), (0,))).astype(BF16)
        for yy in range(4):
            for xx in range(4):
                at = ((yy // 2) * 4 + xx) * 128
                for k in range(4, 6):
                    low = (yy % 2) * 64 + FIRST[k] - 192
                    g_bufs[k][block_at(k, zz, yy, xx)] = out[low : low + 32, at : at + 128]
        out = dot(gproj_ref[t_rows, :], x_ref[...], ((1,), (0,))).astype(BF16)
        for yy in range(4):
            for xx in range(4):
                at = ((yy // 2) * 4 + xx) * 128
                for k in range(4):
                    low = (yy % 2) * 192 + FIRST[k]
                    g_bufs[k][block_at(k, zz, yy, xx)] = out[low : low + 48, at : at + 128]

    def q_part(k, p, s, count):
        n = max(1, (1 << p) // 2)
        return q_bufs[k].at[pl.ds(PIECE_AT[p] + (s - p) * n, count * n)]

    def rs_send(k, s, p):
        at, n = held(across(bits[k], s), p)
        remote(
            g_bufs[k].at[pl.ds(at, n)],
            q_part(k, p, s, 1),
            rs_send_sem.at[k],
            rs_recv.at[k, p],
            order(k)[s],
        ).start()

    def rs_rest(s):
        for p in range(s - 1, -1, -1):
            for k in range(COLOURS):
                rs_send(k, s, p)

    names = tuple(order(0)[::-1]) + ("c",)

    def sum_step(i):
        return remote(sum_ref.at[i], sum_in.at[i], sum_send.at[i], sum_recv.at[i], names[i])

    def sum_finish(i):
        sum_step(i).wait_recv()
        sum_ref[i + 1] = sum_ref[i] + sum_in[i]

    swap.wait()
    scaled = xhat_ref[...]
    grad_normed = gn_own[...] + gn_in[...].astype(F32)
    gn_own[...] = grad_normed
    sum_ref[0] = jnp.concatenate(
        [
            jnp.sum(grad_normed * scaled, axis=0, keepdims=True),
            jnp.sum(grad_normed, axis=0, keepdims=True),
        ],
        axis=0,
    )
    sum_step(0).start()
    for k in range(COLOURS):
        rs_send(k, BITS - 1, BITS - 1)
    rs_rest(BITS - 1)

    live_own = live_ref[own_rows, :][:, :1]
    scaled = xhat_ref[...]
    g = gn_own[...] * gain_ref[...]
    grad_ln = rstd_ref[...][:, :1] * (
        g
        - jnp.mean(g, axis=-1, keepdims=True)
        - scaled * jnp.mean(g * scaled, axis=-1, keepdims=True)
    )
    dtok_ref[...] = (up_ref[...].astype(F32) * live_own + grad_ln).astype(BF16)
    store = pltpu.make_async_copy(dtok_ref, dtok_out, load_sem.at[7])
    store.start()

    for s in range(BITS - 2, -1, -1):
        p = s + 1
        count = BITS - p
        for k in range(COLOURS):
            at, n = held(bits[k], p)
            whole = q_part(k, p, p, count)
            pltpu.make_async_copy(whole, whole, rs_recv.at[k, p]).wait()
            total = g_bufs[k][pl.ds(at, n)].astype(F32)
            for j in range(count):
                first_at = PIECE_AT[p] + j * n
                total = total + q_bufs[k][first_at : first_at + n].astype(F32)
            g_bufs[k][pl.ds(at, n)] = total.astype(BF16)
            if k == 0:
                i = BITS - 2 - s
                sum_finish(i)
                sum_step(i + 1).start()
            rs_send(k, s, s)
        rs_rest(s)
    for k in range(COLOURS):
        whole = q_part(k, 0, 0, BITS)
        pltpu.make_async_copy(whole, whole, rs_recv.at[k, 0]).wait()
        total = g_bufs[k][joined(bits[k])].astype(F32)
        for s in range(BITS):
            total = total + q_bufs[k][s].astype(F32)
        last_own[FIRST[k] : FIRST[k] + ROWS[k]] = total
    final = pair_copy(5, last_own, last_in)
    final.start()
    sum_finish(BITS - 1)
    sum_step(BITS).start()
    sum_finish(BITS)
    sums_ref[...] = sum_ref[BITS + 1]
    store.wait()
    final.wait()
    for h in range(2):
        blk = jnp.where(c == h, last_own[...], last_in[...])
        last_ref[h] = jnp.where(c == 0, blk, pltpu.roll(blk, 64, 1))
    for i in range(BITS + 1):
        sum_step(i).wait_send()
    for k in range(COLOURS):
        for bufs, sems in ((w_bufs, ag_send), (g_bufs, rs_send_sem)):
            part = bufs[k].at[pl.ds(0, BLOCKS - 1)]
            pltpu.make_async_copy(part, part, sems.at[k]).wait()


def finish(dtok_in, last_in, sums_in, dtok_ref, dq_ref, do_ref, dgain_ref, dbias_ref):
    dtok_ref[...] = dtok_in[...]
    for h in range(2):
        blk = last_in[h].T[:64]
        dq_ref[:, 192 * h : 192 * (h + 1)] = blk[:, :192]
        do_ref[:, 64 * h : 64 * (h + 1)] = blk[:, 192:]
    dgain_ref[...] = sums_in[0:1]
    dbias_ref[...] = sums_in[1:2]


def on_device(tokens, upstream, counts, norm_gain, norm_bias, w_qkv, w_out):
    vmem = pl.BlockSpec(memory_space=pltpu.VMEM)
    hbm = pl.BlockSpec(memory_space=pltpu.HBM)
    blocks = [pltpu.VMEM((BLOCKS, r, 128), BF16) for r in ROWS]
    parts = [pltpu.VMEM((BLOCKS - 1, r, 128), BF16) for r in ROWS]
    dma = pltpu.SemaphoreType.DMA
    dtok, last, sums = pl.pallas_call(
        kernel,
        out_shape=(
            jax.ShapeDtypeStruct((256, D), BF16),
            jax.ShapeDtypeStruct((2, 256, 128), F32),
            jax.ShapeDtypeStruct((2, D), F32),
        ),
        in_specs=[hbm] * 7,
        out_specs=(hbm, vmem, vmem),
        scratch_shapes=[
            *blocks,
            *blocks,
            *parts,
            pltpu.VMEM((2, 256, 128), BF16),
            pltpu.VMEM((256, 128), BF16),
            pltpu.VMEM((512, D), BF16),
            pltpu.VMEM((512, D), BF16),
            pltpu.VMEM((512, 128), F32),
            pltpu.VMEM((256, D), F32),
            pltpu.VMEM((256, 128), F32),
            pltpu.VMEM((1536, D), BF16),
            pltpu.VMEM((512, D), BF16),
            pltpu.VMEM((1536, 512), BF16),
            pltpu.VMEM((512, 512), BF16),
            pltpu.VMEM((512, 512), BF16),
            pltpu.VMEM((1536, 512), BF16),
            pltpu.VMEM((256, D), F32),
            pltpu.VMEM((256, D), BF16),
            pltpu.VMEM((256, D), BF16),
            pltpu.VMEM((8, 2, D), F32),
            pltpu.VMEM((7, 2, D), F32),
            pltpu.VMEM((256, 128), F32),
            pltpu.VMEM((256, 128), F32),
            dma((COLOURS,)),
            dma((COLOURS, BITS)),
            dma((COLOURS,)),
            dma((COLOURS, BITS)),
            dma((6,)),
            dma((6,)),
            dma((7,)),
            dma((7,)),
            pltpu.VMEM((256, D), BF16),
            pltpu.VMEM((256, D), BF16),
            pltpu.VMEM((64, 384), BF16),
            pltpu.VMEM((64, 128), BF16),
            pltpu.VMEM((1, D), F32),
            pltpu.VMEM((1, D), F32),
            pltpu.SMEM((32,), jnp.int32),
            pltpu.VMEM((256, D), BF16),
            dma((8,)),
        ],
        compiler_params=pltpu.CompilerParams(
            collective_id=0, has_side_effects=True, vmem_limit_bytes=60 * 1024 * 1024
        ),
    )(
        tokens,
        upstream,
        counts,
        norm_gain.reshape(1, D),
        norm_bias.reshape(1, D),
        w_qkv,
        w_out.T,
    )
    dtok, dq, do, dgain, dbias = pl.pallas_call(
        finish,
        out_shape=(
            jax.ShapeDtypeStruct((256, D), BF16),
            jax.ShapeDtypeStruct((64, 384), F32),
            jax.ShapeDtypeStruct((64, 128), F32),
            jax.ShapeDtypeStruct((1, D), F32),
            jax.ShapeDtypeStruct((1, D), F32),
        ),
        in_specs=[vmem] * 3,
        out_specs=(vmem,) * 5,
        compiler_params=pltpu.CompilerParams(vmem_limit_bytes=60 * 1024 * 1024),
    )(dtok, last, sums)
    return dtok, dq, do.T, dgain.reshape(D), dbias.reshape(D)


def solution(mesh):
    finer = Mesh(
        mesh.devices.reshape(2, 4, 2, 4, 2), ("dp_0", "dp_1", "dp_2", "tensor_0", "tensor_1")
    )
    in_specs = (
        P(DP_TENSOR, None),
        P(DP_TENSOR, None),
        P(DP),
        P(),
        P(),
        P(DP, TENSOR),
        P(TENSOR, DP),
    )
    out_specs = (P(DP_TENSOR, None), P(DP, TENSOR), P(TENSOR, DP), P(), P())
    return jax.shard_map(
        on_device, mesh=finer, in_specs=in_specs, out_specs=out_specs, check_vma=False
    )
```

```python
import functools

import jax
import jax.numpy as jnp
from jax import lax
from jax.experimental import pallas as pl
from jax.experimental.pallas import tpu as pltpu
from jax.sharding import Mesh
from jax.sharding import PartitionSpec as P

D = 1024
HEAD = 64
CAP = 64
TENSOR = ("tensor_0", "tensor_1")
DP = ("dp_0", "dp_1", "dp_2")
DP_TENSOR = ("dp_0", "dp_1", "dp_2", "tensor_0", "tensor_1")
MESH = pl.DeviceIdType.MESH
F32 = jnp.float32
BF16 = jnp.bfloat16

ROWS = (48, 48, 48, 48, 32, 32)
FIRST = (0, 48, 96, 144, 192, 224)
COLOURS = 6
BITS = 6
BASE = ("x0", "y0", "z0", "x1", "y1", "z1")


def order(colour):
    return [BASE[(colour + s) % BITS] for s in range(BITS)]


def gray(x, y, z):
    return {
        "x0": ((x + 1) // 2) % 2,
        "x1": x // 2,
        "y0": ((y + 1) // 2) % 2,
        "y1": y // 2,
        "z0": ((z + 1) // 2) % 2,
        "z1": z // 2,
    }


def bits_of(place, colour):
    return [place[name] for name in order(colour)]


def joined(bits):
    total = 0
    for s, bit in enumerate(bits):
        total = total + bit * (1 << s)
    return total


def held(bits, p, near):
    if p == 0:
        return joined(bits), 1
    if p == 1:
        return joined([1 - bits[0]] + list(bits[1:])), 1
    low = bits[p - 2] if near else 1 - bits[p - 2]
    return joined([0] * (p - 2) + [low, 1 - bits[p - 1]] + list(bits[p:])), 1 << (p - 2)


def kinds(p):
    return (0, 1) if p > 1 else (0,)


def across(bits, s):
    return list(bits[:s]) + [1 - bits[s]] + list(bits[s + 1 :])


PIECE_AT = {}
_at = 0
for _p in range(BITS):
    for _near in kinds(_p):
        PIECE_AT[_p, _near] = _at
        _at += (BITS - _p) << max(0, _p - 2)

EVENTS = [(BITS, 0)]
for _p in range(BITS - 1, 0, -1):
    EVENTS += [(_p, near) for near in kinds(_p)]


def issue_event(s, p, near):
    ready = 0 if s == BITS - 1 else EVENTS.index((s + 1, int(p < s)))
    due = min(BITS, p + 1 if near else p + 2)
    return max(ready, EVENTS.index((due, 0)))


ISSUES = {event: [] for event in EVENTS}
for _s in range(BITS):
    for _p in range(_s, -1, -1):
        for _near in kinds(_p):
            ISSUES[EVENTS[issue_event(_s, _p, _near)]].append((_s, _p, _near))
for _event in EVENTS:
    ISSUES[_event].sort(key=lambda e: (e[0] != _event[0] - 1 or e[1] != e[0], -e[1], e[2]))

BLOCKS = 1 << BITS


def dot(a, b, dims):
    return lax.dot_general(a, b, (dims, ((), ())), preferred_element_type=F32)


def kernel(
    tok_in,
    up_in,
    counts_in,
    gain_in,
    bias_in,
    wq_in,
    wo_in,
    dtok_out,
    last_ref,
    sums_ref,
    *scratch,
):
    w_bufs = scratch[0:6]
    g_bufs = scratch[6:12]
    q_bufs = scratch[12:18]
    (
        mine,
        theirs,
        x_ref,
        u_ref,
        live_ref,
        xhat_ref,
        rstd_ref,
        wt_ref,
        wot_ref,
        proj_ref,
        gatt_ref,
        att_ref,
        gproj_ref,
        gn_own,
        gn_out,
        gn_in,
        sum_ref,
        sum_in,
        last_own,
        last_in,
        ag_send,
        ag_recv,
        rs_send_sem,
        rs_recv,
        pair_send,
        pair_recv,
        sum_send,
        sum_recv,
        tok_ref,
        up_ref,
        wq_ref,
        wo_ref,
        gain_ref,
        bias_ref,
        counts_ref,
        dtok_ref,
        score_ref,
        gprob_ref,
        key_ref,
        pair_ref,
        load_sem,
    ) = scratch[18:]

    loads = [
        pltpu.make_async_copy(wq_in, wq_ref, load_sem.at[0]),
        pltpu.make_async_copy(wo_in, wo_ref, load_sem.at[1]),
        pltpu.make_async_copy(tok_in, tok_ref, load_sem.at[2]),
        pltpu.make_async_copy(up_in, up_ref, load_sem.at[3]),
        pltpu.make_async_copy(gain_in, gain_ref, load_sem.at[4]),
        pltpu.make_async_copy(bias_in, bias_ref, load_sem.at[5]),
        pltpu.make_async_copy(counts_in, counts_ref, load_sem.at[6]),
    ]
    for load in loads:
        load.start()

    yh, x, c = (lax.axis_index(name) for name in DP)
    z, yl = (lax.axis_index(name) for name in TENSOR)
    y = 2 * yh + yl
    place = gray(x, y, z)
    peer = {
        "x0": {"dp_1": x + 1 - 2 * (x % 2)},
        "x1": {"dp_1": 3 - x},
        "y0": {"tensor_1": 1 - yl},
        "y1": {"dp_0": 1 - yh, "tensor_1": 1 - yl},
        "z0": {"tensor_0": z + 1 - 2 * (z % 2)},
        "z1": {"tensor_0": 3 - z},
        "c": {"dp_2": 1 - c},
    }
    bits = [bits_of(place, k) for k in range(COLOURS)]

    barrier = pltpu.get_barrier_semaphore()
    for name in peer:
        pl.semaphore_signal(barrier, inc=1, device_id=peer[name], device_id_type=MESH)

    def remote(src, dst, send, recv, name):
        return pltpu.make_async_remote_copy(
            src_ref=src,
            dst_ref=dst,
            send_sem=send,
            recv_sem=recv,
            device_id=peer[name],
            device_id_type=MESH,
        )

    def pair_copy(i, src, dst):
        return remote(src, dst, pair_send.at[i], pair_recv.at[i], "c")

    loads[0].wait()
    loads[1].wait()
    wq_t = wq_ref[...].astype(F32).T
    wo_f = wo_ref[...].astype(F32).T
    for h in range(2):
        part = jnp.concatenate(
            [wq_t[192 * h : 192 * (h + 1)], wo_f[64 * h : 64 * (h + 1)]], axis=0
        )
        mine[h] = jnp.concatenate([part, part], axis=1).astype(BF16)

    pl.semaphore_wait(barrier, len(peer))
    first = pair_copy(0, mine.at[1 - c], theirs)
    first.start()
    first.wait()
    lane = lax.broadcasted_iota(jnp.int32, (256, 128), 1)
    own_half = (lane < 64) == (c == 0)
    block = jnp.where(own_half, mine[c].astype(F32), theirs[...].astype(F32)).astype(BF16)
    for k in range(COLOURS):
        w_bufs[k][joined(bits[k])] = block[FIRST[k] : FIRST[k] + ROWS[k]]

    def ag_send_part(k, s, p, near):
        at, n = held(bits[k], p, near)
        part = w_bufs[k].at[pl.ds(at, n)]
        sem = ag_recv.at[k, 2 * s + (p < s)]
        remote(part, part, ag_send.at[k], sem, order(k)[s]).start()

    def ag_event(p, near):
        for k in range(COLOURS):
            if p > 0:
                at, n = held(bits[k], p, near)
                part = w_bufs[k].at[pl.ds(at, n)]
                sem = ag_recv.at[k, 2 * (p - 1) + near]
                pltpu.make_async_copy(part, part, sem).wait()
            if p < BITS:
                ag_send_part(k, p, p, near)
        for s in range(p + 1, BITS):
            for k in range(COLOURS):
                ag_send_part(k, s, p, near)

    ag_event(0, 0)

    for load in loads[2:]:
        load.wait()
    values = tok_ref[...].astype(F32)
    centre = jnp.mean(values, axis=-1, keepdims=True)
    shifted = values - centre
    variance = jnp.mean(shifted * shifted, axis=-1, keepdims=True)
    inverse = lax.rsqrt(variance + 1e-6)
    scaled = shifted * inverse
    xhat_ref[...] = scaled
    rstd_ref[...] = jnp.broadcast_to(inverse, (256, 128))
    own_rows = pl.ds(pl.multiple_of(c * 256, 256), 256)
    x_ref[own_rows, :] = (scaled * gain_ref[...] + bias_ref[...]).astype(BF16)
    start = (2 * z + yl) * 4
    row = lax.broadcasted_iota(jnp.int32, (256, 128), 0)
    image = row // CAP
    count = jnp.where(
        image < 2,
        jnp.where(image == 0, counts_ref[start], counts_ref[start + 1]),
        jnp.where(image == 2, counts_ref[start + 2], counts_ref[start + 3]),
    )
    live = jnp.where(row % CAP < count, 1.0, 0.0).astype(F32)
    live_ref[own_rows, :] = live
    u_ref[own_rows, :] = (up_ref[...].astype(F32) * live[:, :1]).astype(BF16)
    shared = [
        pair_copy(1, x_ref.at[own_rows], x_ref.at[own_rows]),
        pair_copy(2, u_ref.at[own_rows], u_ref.at[own_rows]),
        pair_copy(3, live_ref.at[own_rows], live_ref.at[own_rows]),
    ]
    for copy in shared:
        copy.start()

    for p in range(1, BITS + 1):
        for near in kinds(p)[::-1]:
            ag_event(p, near)

    def block_at(k, zz, yy, xx):
        return joined(bits_of(gray(xx, yy, zz), k))

    @pl.loop(0, 4)
    def _(zz):
        for yy in range(4):
            t_rows = pl.multiple_of((2 * zz + yy % 2) * 192, 192)
            o_rows = pl.multiple_of((2 * zz + yy % 2) * 64, 64)
            for xx in range(4):
                at = ((yy // 2) * 4 + xx) * 128
                for k in range(4):
                    wt_ref[pl.ds(t_rows + FIRST[k], 48), at : at + 128] = w_bufs[k][
                        block_at(k, zz, yy, xx)
                    ]
                for k in range(4, 6):
                    wot_ref[pl.ds(o_rows + FIRST[k] - 192, 32), at : at + 128] = w_bufs[k][
                        block_at(k, zz, yy, xx)
                    ]

    for copy in shared:
        copy.wait()

    @pl.loop(0, 4)
    def _(i):
        rows = pl.ds(pl.multiple_of(i * 384, 384), 384)
        proj_ref[rows, :] = dot(wt_ref[rows, :], x_ref[...], ((1,), (1,))).astype(BF16)

    @pl.loop(0, 2)
    def _(i):
        rows = pl.ds(pl.multiple_of(i * 256, 256), 256)
        gatt_ref[rows, :] = dot(wot_ref[rows, :], u_ref[...], ((1,), (1,))).astype(BF16)

    left = lax.broadcasted_iota(jnp.int32, (64, 128), 1) < 64

    def folded(a):
        return jnp.where(left, a[:64], a[64:])

    def unfolded(a):
        zero = jnp.zeros_like(a)
        both = [jnp.where(left, a, zero), jnp.where(left, zero, a)]
        return jnp.concatenate(both, axis=0).astype(BF16)

    pairs = [slice(128 * pair, 128 * pair + 128) for pair in range(4)]

    @pl.loop(0, 8, unroll=4)
    def _(t):
        base = pl.multiple_of(t * 192, 192)
        o_base = pl.multiple_of(t * 64, 64)
        zero = jnp.zeros((64, 128), BF16)
        for lanes in pairs:
            q = proj_ref[pl.ds(base, 64), lanes]
            kv = proj_ref[pl.ds(base + 64, 128), lanes]
            g = gatt_ref[pl.ds(o_base, 64), lanes]
            top = jnp.concatenate([q, zero], axis=1)
            low = jnp.concatenate([zero, g], axis=1)
            both = dot(kv, jnp.concatenate([top, low], axis=0), ((0,), (0,)))
            score_ref[t, :, lanes] = folded(both[:, :128])
            gprob_ref[t, :, lanes] = folded(both[:, 128:])

    alive = [folded(live_ref[lanes, :]) for lanes in pairs]
    key_ref[...] = jnp.concatenate(alive, axis=1)

    @pl.loop(0, 8, unroll=2)
    def _(t):
        scores = jnp.where(key_ref[...] > 0.5, score_ref[t] * 0.125, -1e30)
        powers = jnp.exp(scores - jnp.max(scores, axis=0, keepdims=True))
        probs = powers * (1.0 / jnp.sum(powers, axis=0, keepdims=True))
        grad_probs = gprob_ref[t]
        delta = jnp.sum(probs * grad_probs, axis=0, keepdims=True)
        grad_scores = probs * (grad_probs - delta) * 0.125
        for i, lanes in enumerate(pairs):
            pair_ref[t, i, :, 0:128] = unfolded(grad_scores[:, lanes])
            pair_ref[t, i, :, 128:256] = unfolded(probs[:, lanes])


    @pl.loop(0, 8, unroll=4)
    def _(t):
        base = pl.multiple_of(t * 192, 192)
        o_base = pl.multiple_of(t * 64, 64)
        for i, lanes in enumerate(pairs):
            q = proj_ref[pl.ds(base, 64), lanes]
            kv = proj_ref[pl.ds(base + 64, 128), lanes]
            g = gatt_ref[pl.ds(o_base, 64), lanes]
            out = dot(kv, pair_ref[t, i], ((1,), (0,))).astype(BF16)
            gproj_ref[pl.ds(base, 64), lanes] = out[:64, :128]
            att_ref[pl.ds(o_base, 64), lanes] = out[64:, 128:]
            tall = jnp.concatenate([pair_ref[t, i, :, 0:128], pair_ref[t, i, :, 128:256]], axis=0)
            out = dot(jnp.concatenate([q, g], axis=0), tall, ((1,), (1,))).astype(BF16)
            gproj_ref[pl.ds(base + 64, 64), lanes] = out[:64, :128]
            gproj_ref[pl.ds(base + 128, 64), lanes] = out[64:, 128:]

    swap = pair_copy(4, gn_out, gn_in)
    for other in (1, 0):
        for half in range(2):
            rows = pl.ds(
                pl.multiple_of((c if other == 0 else 1 - c) * 256 + half * 128, 128), 128
            )
            part = dot(gproj_ref[:, rows], wt_ref[...], ((0,), (0,)))
            if other == 0:
                gn_own[half * 128 : half * 128 + 128] = part
            else:
                gn_out[half * 128 : half * 128 + 128] = part.astype(BF16)
        if other == 1:
            swap.start()

    @pl.loop(0, 4)
    def _(zz):
        o_rows = pl.ds(pl.multiple_of(zz * 128, 128), 128)
        t_rows = pl.ds(pl.multiple_of(zz * 384, 384), 384)
        out = dot(att_ref[o_rows, :], u_ref[...], ((1,), (0,))).astype(BF16)
        for yy in range(4):
            for xx in range(4):
                at = ((yy // 2) * 4 + xx) * 128
                for k in range(4, 6):
                    low = (yy % 2) * 64 + FIRST[k] - 192
                    g_bufs[k][block_at(k, zz, yy, xx)] = out[low : low + 32, at : at + 128]
        out = dot(gproj_ref[t_rows, :], x_ref[...], ((1,), (0,))).astype(BF16)
        for yy in range(4):
            for xx in range(4):
                at = ((yy // 2) * 4 + xx) * 128
                for k in range(4):
                    low = (yy % 2) * 192 + FIRST[k]
                    g_bufs[k][block_at(k, zz, yy, xx)] = out[low : low + 48, at : at + 128]

    def q_part(k, p, near, s, count):
        n = 1 << max(0, p - 2)
        return q_bufs[k].at[pl.ds(PIECE_AT[p, near] + (s - p) * n, count * n)]

    def rs_send(k, s, p, near):
        at, n = held(across(bits[k], s), p, near)
        remote(
            g_bufs[k].at[pl.ds(at, n)],
            q_part(k, p, near, s, 1),
            rs_send_sem.at[k],
            rs_recv.at[k, 2 * p + near],
            order(k)[s],
        ).start()

    def rs_wait(k, p, near):
        whole = q_part(k, p, near, p, BITS - p)
        pltpu.make_async_copy(whole, whole, rs_recv.at[k, 2 * p + near]).wait()

    def rs_issue(event, ks, first):
        for s, p, near in ISSUES[event]:
            if (s == event[0] - 1 and p == s) == first:
                for k in ks:
                    rs_send(k, s, p, near)

    names = tuple(order(0)[::-1]) + ("c",)

    def sum_step(i):
        return remote(sum_ref.at[i], sum_in.at[i], sum_send.at[i], sum_recv.at[i], names[i])

    def sum_finish(i):
        sum_step(i).wait_recv()
        sum_ref[i + 1] = sum_ref[i] + sum_in[i]

    swap.wait()
    scaled = xhat_ref[...]
    grad_normed = gn_own[...] + gn_in[...].astype(F32)
    gn_own[...] = grad_normed
    sum_ref[0] = jnp.concatenate(
        [
            jnp.sum(grad_normed * scaled, axis=0, keepdims=True),
            jnp.sum(grad_normed, axis=0, keepdims=True),
        ],
        axis=0,
    )
    sum_step(0).start()
    rs_issue((BITS, 0), range(COLOURS), True)
    rs_issue((BITS, 0), range(COLOURS), False)

    live_own = live_ref[own_rows, :][:, :1]
    scaled = xhat_ref[...]
    g = gn_own[...] * gain_ref[...]
    grad_ln = rstd_ref[...][:, :1] * (
        g
        - jnp.mean(g, axis=-1, keepdims=True)
        - scaled * jnp.mean(g * scaled, axis=-1, keepdims=True)
    )
    dtok_ref[...] = (up_ref[...].astype(F32) * live_own + grad_ln).astype(BF16)
    store = pltpu.make_async_copy(dtok_ref, dtok_out, load_sem.at[7])
    store.start()

    for event in EVENTS[1:]:
        p, near = event
        for k in range(COLOURS):
            rs_wait(k, p, near)
            at, n = held(bits[k], p, near)
            total = g_bufs[k][pl.ds(at, n)].astype(F32)
            for j in range(BITS - p):
                first_at = PIECE_AT[p, near] + j * n
                total = total + q_bufs[k][first_at : first_at + n].astype(F32)
            g_bufs[k][pl.ds(at, n)] = total.astype(BF16)
            if k == 0 and near == 0:
                i = BITS - 1 - p
                sum_finish(i)
                sum_step(i + 1).start()
            rs_issue(event, (k,), True)
        rs_issue(event, range(COLOURS), False)
    for k in range(COLOURS):
        rs_wait(k, 0, 0)
        total = g_bufs[k][joined(bits[k])].astype(F32)
        for s in range(BITS):
            total = total + q_bufs[k][s].astype(F32)
        last_own[FIRST[k] : FIRST[k] + ROWS[k]] = total
    final = pair_copy(5, last_own, last_in)
    final.start()
    sum_finish(BITS - 1)
    sum_step(BITS).start()
    sum_finish(BITS)
    sums_ref[...] = sum_ref[BITS + 1]
    store.wait()
    final.wait()
    for h in range(2):
        blk = jnp.where(c == h, last_own[...], last_in[...])
        last_ref[h] = jnp.where(c == 0, blk, pltpu.roll(blk, 64, 1))
    for i in range(BITS + 1):
        sum_step(i).wait_send()
    for k in range(COLOURS):
        for bufs, sems in ((w_bufs, ag_send), (g_bufs, rs_send_sem)):
            part = bufs[k].at[pl.ds(0, BLOCKS - 1)]
            pltpu.make_async_copy(part, part, sems.at[k]).wait()


def finish(dtok_in, last_in, sums_in, dtok_ref, dq_ref, do_ref, dgain_ref, dbias_ref):
    dtok_ref[...] = dtok_in[...]
    for h in range(2):
        blk = last_in[h].T[:64]
        dq_ref[:, 192 * h : 192 * (h + 1)] = blk[:, :192]
        do_ref[:, 64 * h : 64 * (h + 1)] = blk[:, 192:]
    dgain_ref[...] = sums_in[0:1]
    dbias_ref[...] = sums_in[1:2]


def on_device(tokens, upstream, counts, norm_gain, norm_bias, w_qkv, w_out):
    vmem = pl.BlockSpec(memory_space=pltpu.VMEM)
    hbm = pl.BlockSpec(memory_space=pltpu.HBM)
    blocks = [pltpu.VMEM((BLOCKS, r, 128), BF16) for r in ROWS]
    parts = [pltpu.VMEM((BLOCKS - 1, r, 128), BF16) for r in ROWS]
    dma = pltpu.SemaphoreType.DMA
    dtok, last, sums = pl.pallas_call(
        kernel,
        out_shape=(
            jax.ShapeDtypeStruct((256, D), BF16),
            jax.ShapeDtypeStruct((2, 256, 128), F32),
            jax.ShapeDtypeStruct((2, D), F32),
        ),
        in_specs=[hbm] * 7,
        out_specs=(hbm, vmem, vmem),
        scratch_shapes=[
            *blocks,
            *blocks,
            *parts,
            pltpu.VMEM((2, 256, 128), BF16),
            pltpu.VMEM((256, 128), BF16),
            pltpu.VMEM((512, D), BF16),
            pltpu.VMEM((512, D), BF16),
            pltpu.VMEM((512, 128), F32),
            pltpu.VMEM((256, D), F32),
            pltpu.VMEM((256, 128), F32),
            pltpu.VMEM((1536, D), BF16),
            pltpu.VMEM((512, D), BF16),
            pltpu.VMEM((1536, 512), BF16),
            pltpu.VMEM((512, 512), BF16),
            pltpu.VMEM((512, 512), BF16),
            pltpu.VMEM((1536, 512), BF16),
            pltpu.VMEM((256, D), F32),
            pltpu.VMEM((256, D), BF16),
            pltpu.VMEM((256, D), BF16),
            pltpu.VMEM((8, 2, D), F32),
            pltpu.VMEM((7, 2, D), F32),
            pltpu.VMEM((256, 128), F32),
            pltpu.VMEM((256, 128), F32),
            dma((COLOURS,)),
            dma((COLOURS, 2 * BITS)),
            dma((COLOURS,)),
            dma((COLOURS, 2 * BITS)),
            dma((6,)),
            dma((6,)),
            dma((7,)),
            dma((7,)),
            pltpu.VMEM((256, D), BF16),
            pltpu.VMEM((256, D), BF16),
            pltpu.VMEM((64, 384), BF16),
            pltpu.VMEM((64, 128), BF16),
            pltpu.VMEM((1, D), F32),
            pltpu.VMEM((1, D), F32),
            pltpu.SMEM((32,), jnp.int32),
            pltpu.VMEM((256, D), BF16),
            pltpu.VMEM((8, 64, 512), F32),
            pltpu.VMEM((8, 64, 512), F32),
            pltpu.VMEM((64, 512), F32),
            pltpu.VMEM((8, 4, 128, 256), BF16),
            dma((8,)),
        ],
        compiler_params=pltpu.CompilerParams(
            collective_id=0, has_side_effects=True, vmem_limit_bytes=60 * 1024 * 1024
        ),
    )(
        tokens,
        upstream,
        counts,
        norm_gain.reshape(1, D),
        norm_bias.reshape(1, D),
        w_qkv,
        w_out.T,
    )
    dtok, dq, do, dgain, dbias = pl.pallas_call(
        finish,
        out_shape=(
            jax.ShapeDtypeStruct((256, D), BF16),
            jax.ShapeDtypeStruct((64, 384), F32),
            jax.ShapeDtypeStruct((64, 128), F32),
            jax.ShapeDtypeStruct((1, D), F32),
            jax.ShapeDtypeStruct((1, D), F32),
        ),
        in_specs=[vmem] * 3,
        out_specs=(vmem,) * 5,
        compiler_params=pltpu.CompilerParams(vmem_limit_bytes=60 * 1024 * 1024),
    )(dtok, last, sums)
    return dtok, dq, do.T, dgain.reshape(D), dbias.reshape(D)


def solution(mesh):
    finer = Mesh(
        mesh.devices.reshape(2, 4, 2, 4, 2), ("dp_0", "dp_1", "dp_2", "tensor_0", "tensor_1")
    )
    in_specs = (
        P(DP_TENSOR, None),
        P(DP_TENSOR, None),
        P(DP),
        P(),
        P(),
        P(DP, TENSOR),
        P(TENSOR, DP),
    )
    out_specs = (P(DP_TENSOR, None), P(DP, TENSOR), P(TENSOR, DP), P(), P())
    return jax.shard_map(
        on_device, mesh=finer, in_specs=in_specs, out_specs=out_specs, check_vma=False
    )
```
